32 devices in a mesh: grp: 4 (over y, x), mem: 8 (over z, core).
Axes of the slice: x: 2, y: 2, z: 4, core: 2. Of those that a mesh axis runs over, the one named last changes fastest.
Arguments:
- embeddings: bfloat16 [4096, 1024], P(('grp', 'mem')), may hold values from -6 to 6
- cluster: int32 [4096, 1], P(('grp', 'mem')), may hold values from 0 to 3; in each aligned block of 128 rows (0 to 127, 128 to 255, ...) at most 64 rows name the same one
- rank: int32 [4096], P(('grp', 'mem')), may hold values from 0 to 1048575
Outputs:
- similarity: float32 [4096], P(('grp', 'mem'))
The draws below stay inside these ranges and needn't reach their ends.
Inputs may be any that keep to these rules, and one draw needn't show every extreme that they name: `cluster`: in each aligned block of 128 rows (the rows of one device) no group is named by more than 64 rows. A smaller rank is earlier; equal ranks are not earlier.
All inputs are finite; a program needn't handle non-finite values.
Results may differ from the reference program's by a relative error of at most 0.0013.
Values may be sent and summed in bfloat16 or wider, within the bound.
No kernel may reach another device: no remote copies, remote signals or barrier semaphores. Data moves between devices by JAX's collectives and lax.ppermute only.
A program may use at most 64 MiB of HBM per device.

```python
import math
import jax
import jax.numpy as jnp
import numpy as np
from jax import lax

D = 1024
ROWS_DEV = 128
CAP = 64
POINTS = 4096
N_GRP = 4
N_MEM = 8


def place_ends(array, key, smallest, top_value):
    index_at = [jax.random.randint(jax.random.fold_in(key, axis), (), 0, length) for axis, length in enumerate(array.shape)]
    widest = array.shape.index(max(array.shape))
    beside = index_at[:widest] + [(index_at[widest] + 1) % array.shape[widest]] + index_at[widest + 1:]
    return array.at[tuple(index_at)].set(smallest).at[tuple(beside)].set(top_value)


def steps_of(own_key, extent, cuts, least, top_value):
    level, own = 1.0, jax.random.fold_in(own_key, 6)
    for position, shards_of in cuts:
        draws = jnp.exp(jax.random.uniform(jax.random.fold_in(own, position), (shards_of,), jnp.float32, least / len(cuts), top_value / len(cuts)))
        level = level * jnp.repeat(draws, extent[position] // shards_of).reshape([-1 if axis == position else 1 for axis in range(len(extent))])
    return level


def deal_out(rng, own, number, rows, amount, top, limit, skew):
    order = jax.random.permutation(rng, amount)
    heavy_load, ordinary = shares(amount, rows * top, limit, skew, True), shares(amount, rows * top, limit, skew, False)
    places = jnp.arange(amount)

    def named(sizes, offset_by):
        used = int((sizes > 0).sum())
        fixed = max(1, used // 4)
        moved = fixed + (places - fixed + offset_by * (used - fixed)) % max(1, amount - fixed)
        return jnp.zeros((amount,), jnp.int32).at[order[jnp.where(places < fixed, places, moved)]].set(jnp.asarray(sizes, jnp.int32))

    sizes = jnp.where(number % 4 == 0, named(heavy_load, number // 4), named(ordinary, number - number // 4 - 1))
    mixed = jax.random.permutation(jax.random.fold_in(own, 3), amount)
    giver, taker = mixed[0:amount // 2 * 2:2], mixed[1:amount // 2 * 2:2]
    room = jnp.minimum(sizes[giver] - 1, limit - sizes[taker]) // 2
    room = jnp.where((giver == order[0]) | (taker == order[0]) | (sizes[taker] == 0), 0, jnp.maximum(room, 0))
    moved = jax.random.randint(jax.random.fold_in(own, 4), (amount // 2,), 0, 1 << 20) % (room + 1)
    sizes = sizes.at[giver].add(-moved).at[taker].add(moved)
    labels = jnp.searchsorted(jnp.cumsum(sizes), jnp.arange(rows * top), side="right").astype(jnp.int32)
    listing = labels.reshape(top, rows).T
    listing = listing[jax.random.permutation(jax.random.fold_in(own, 1), rows)]
    offset_by = jax.random.randint(jax.random.fold_in(own, 2), (rows, 1), 0, top)
    return jnp.take_along_axis(listing, (jnp.arange(top)[None, :] + offset_by) % top, axis=1)


def shares(amount, total, reach, lean, full):
    portions = [(1 << 20) // math.isqrt(grade ** lean) + 1 for grade in range(1, amount + 1)]
    largest = reach if full else min(reach, max(-(-total // amount), total * portions[0] // sum(portions)))
    least = 1 if total - largest >= amount - 1 else 0
    counts, spare = [largest] + [least] * (amount - 1), total - largest - least * (amount - 1)
    while spare > 0:
        candidates = [i for i in range(1, amount) if counts[i] < largest] or [i for i in range(1, amount) if counts[i] < reach]
        mass, left = sum([portions[i] for i in candidates]), spare
        for i in candidates:
            addition = min(reach - counts[i], max(1, left * portions[i] // mass), spare)
            counts[i] = counts[i] + addition
            spare = spare - addition
    return np.array(counts)


def noise(rng, dims, width, most, cuts=(), kind=jnp.bfloat16):
    gain = steps_of(rng, dims, cuts, -0.22, 0.18) if cuts else 1.0
    drawn = jax.random.normal(rng, dims, jnp.float32) * width * gain
    return jnp.minimum(jnp.maximum(drawn, -most), most).astype(kind)


def setup_inputs(seed: int = 0) -> dict:
    keys = jax.random.split(jax.random.key(seed), 4)
    embeddings = noise(keys[0], (POINTS, D), 1.0, 6.0, ((0, 32),))
    cluster_keys = jax.random.split(jax.random.fold_in(keys[1], 1), POINTS // ROWS_DEV)
    cluster_turns = jax.random.permutation(jax.random.fold_in(keys[1], 3), POINTS // ROWS_DEV)
    cluster = jax.vmap(lambda own, number: deal_out(jax.random.fold_in(keys[1], 2), own, number, ROWS_DEV, N_GRP, 1, CAP, 2))(cluster_keys, cluster_turns).reshape((POINTS, 1))
    rank = place_ends(jax.random.randint(keys[2], (POINTS,), 0, 1048576), jax.random.fold_in(keys[2], 1), 0, 1048575).astype(jnp.int32)
    return {"embeddings": embeddings, "cluster": cluster, "rank": rank}


def reference(embeddings, cluster, rank):
    wide = embeddings.astype(jnp.float32)
    normed = (wide * lax.rsqrt(lax.optimization_barrier(jnp.sum(wide * wide, axis=1, keepdims=True)) + 1e-06)).astype(jnp.bfloat16)
    owner = cluster[:, 0].astype(jnp.int32)
    sort_key = owner * 2097152 + rank
    order = jnp.argsort(sort_key, stable=True).astype(jnp.int32)
    span = N_GRP * N_MEM * CAP
    block = math.gcd(POINTS, 512)
    sorted_keys = jnp.concatenate([jnp.zeros((span, D), jnp.bfloat16), normed[order]], axis=0)
    sorted_owner = jnp.concatenate([jnp.full((span,), -1, jnp.int32), owner[order]], axis=0)
    sorted_rank = jnp.concatenate([jnp.zeros((span,), jnp.int32), rank[order]], axis=0)

    def one_block(index):
        start = (index * block).astype(jnp.int32)
        queries = lax.dynamic_slice_in_dim(sorted_keys, start + span, block, 0)
        query_owner = lax.dynamic_slice_in_dim(sorted_owner, start + span, block, 0)
        query_rank = lax.dynamic_slice_in_dim(sorted_rank, start + span, block, 0)
        window = lax.dynamic_slice_in_dim(sorted_keys, start, span + block, 0)
        window_owner = lax.dynamic_slice_in_dim(sorted_owner, start, span + block, 0)
        window_rank = lax.dynamic_slice_in_dim(sorted_rank, start, span + block, 0)
        gram = jnp.dot(queries, window.T, preferred_element_type=jnp.float32)
        earlier = (window_owner[None, :] == query_owner[:, None]) & (window_rank[None, :] < query_rank[:, None])
        return lax.optimization_barrier(jnp.max(jnp.where(earlier, gram, jnp.float32(-1.0)), axis=1))
    values = lax.map(one_block, jnp.arange(POINTS // block, dtype=jnp.int32)).reshape(POINTS)
    return jnp.zeros((POINTS,), jnp.float32).at[order].set(values)
```

```python
import functools

import jax
import jax.numpy as jnp
from jax import lax
from jax.experimental import pallas as pl
from jax.experimental.pallas import tpu as pltpu
from jax.sharding import PartitionSpec as P

META = 8
SHIFT = 21


def meeting_slots(count):
    load = {}
    slots = []

    def path(a, b):
        step = 1 if b > a else -1
        return [(i, i + step) for i in range(a, b, step)]

    for distance in range(1, count):
        for low in range(count - distance):
            best = None
            for a, b in ((low, low + distance), (low + distance, low)):
                links = [load.get(link, 0) + 1 for link in path(a, b)]
                first = 0 if distance == 1 else 1
                index = first
                while index < len(slots) and any(a == s or b == t for s, t in slots[index]):
                    index += 1
                score = (index >= len(slots), max(links), sum(links), index)
                if best is None or score < best[0]:
                    best = (score, index, a, b)
            _, index, a, b = best
            while len(slots) <= index:
                slots.append([])
            slots[index].append((a, b))
            for link in path(a, b):
                load[link] = load.get(link, 0) + 1
    return [slot for slot in slots if slot]


def prepare_kernel(x_ref, cluster_ref, rank_ref, out_ref):
    rows = x_ref.shape[0]
    wide = x_ref[...].astype(jnp.float32)
    scale = lax.rsqrt(jnp.sum(wide * wide, axis=1, keepdims=True) + 1e-06)
    out_ref[0:rows, :] = (wide * scale).astype(jnp.bfloat16)
    key = cluster_ref[...] * (1 << SHIFT) + rank_ref[...] + 1
    digit = lax.broadcasted_iota(jnp.int32, (META, rows), 0)
    spread = jnp.where(
        digit == 0,
        key & 255,
        jnp.where(digit == 1, (key >> 8) & 255, jnp.where(digit == 2, key >> 16, 0)),
    )
    out_ref[rows : rows + META, :] = jnp.zeros((META, out_ref.shape[1]), jnp.bfloat16)
    out_ref[rows : rows + META, 0:rows] = spread.astype(jnp.float32).astype(jnp.bfloat16)


def keys_of(ref, rows):
    meta = ref[rows : rows + META, 0:rows].astype(jnp.float32)
    key = meta[0:1] + 256.0 * meta[1:2] + 65536.0 * meta[2:3]
    owner = jnp.where(key > 0.0, jnp.floor(meta[2:3] * (1.0 / 32.0)), -1.0)
    return key, owner


def column(row):
    size = row.shape[1]
    return jnp.broadcast_to(row, (size, size)).T


def similarity_kernel(n_query, n_local, cores, groups, members, sources, *refs):
    blocks, out_ref = refs[:-1], refs[-1]
    queries, others = blocks[:n_query], blocks[n_query:]
    rows = queries[0].shape[0] - META
    grp = lax.axis_index("grp")
    mem = lax.axis_index("mem")
    chip = mem // cores
    slot_of = lax.broadcasted_iota(jnp.int32, out_ref.shape, 0)
    result = jnp.full(out_ref.shape, -1.0, jnp.float32)
    query_rows = jnp.concatenate([q[0:rows, :] for q in queries], axis=0)
    query_keys = []
    for q in queries:
        key, owner = keys_of(q, rows)
        query_keys.append((column(key), column(owner)))
    best = [jnp.full((rows, rows), -1.0, jnp.float32) for _ in queries]
    for start in range(0, len(others), cores):
        pair = others[start : start + cores]
        other_rows = jnp.concatenate([k[0:rows, :] for k in pair], axis=0)
        gram = lax.dot_general(
            query_rows,
            other_rows,
            (((1,), (1,)), ((), ())),
            preferred_element_type=jnp.float32,
        )
        for c, k in enumerate(pair):
            key, owner = keys_of(k, rows)
            back = jnp.full((rows, rows), -1.0, jnp.float32)
            for j in range(n_query):
                tile = gram[j * rows : (j + 1) * rows, c * rows : (c + 1) * rows]
                query_key, query_owner = query_keys[j]
                same = owner == query_owner
                best[j] = jnp.maximum(
                    best[j], jnp.where(same & (key < query_key), tile, -1.0)
                )
                if start >= n_local:
                    back = jnp.maximum(
                        back, jnp.where(same & (query_key < key), tile, -1.0)
                    )
            if start >= n_local:
                table = sources[(start - n_local) // cores]
                place = jnp.int32(-1)
                for target, source in table:
                    place = jnp.where(
                        chip == target,
                        grp * members + source * cores
                        + (mem % cores if c == 0 else cores - 1 - mem % cores),
                        place,
                    )
                result = jnp.maximum(
                    result,
                    jnp.where(
                        slot_of == place, jnp.max(back, axis=0, keepdims=True), -1.0
                    ),
                )
    for j in range(n_query):
        place = jnp.bitwise_xor(grp, j) * members + mem
        result = jnp.maximum(
            result,
            jnp.where(
                slot_of == place, jnp.max(best[j].T, axis=0, keepdims=True), -1.0
            ),
        )
    out_ref[...] = result


def body(embeddings, cluster, rank):
    rows, width = embeddings.shape
    groups = lax.axis_size("grp")
    members = lax.axis_size("mem")
    cores = 2 if members % 2 == 0 else 1
    chips = members // cores
    vmem = pl.BlockSpec(memory_space=pltpu.VMEM)
    block = pl.pallas_call(
        prepare_kernel,
        out_shape=jax.ShapeDtypeStruct((rows + META, width), jnp.bfloat16),
        in_specs=[vmem] * 3,
        out_specs=vmem,
        name="prepare",
    )(embeddings, cluster.reshape(1, rows), rank.reshape(1, rows))

    def beside(value):
        if cores == 1:
            return []
        return [lax.ppermute(value, "mem", [(m, m ^ 1) for m in range(members)])]

    slots = meeting_slots(chips)
    others = []
    for slot in slots:
        route = [(a * cores + c, b * cores + c) for a, b in slot for c in range(cores)]
        others.append(lax.ppermute(block, "mem", route))
    queries = [block]
    for distance in range(1, groups):
        queries.append(
            lax.ppermute(block, "grp", [(g, g ^ distance) for g in range(groups)])
        )
    local = [block] + beside(block)
    remote = []
    for other in others:
        remote += [other] + beside(other)
    sources = [[(b, a) for a, b in slot] for slot in slots]
    devices = groups * members
    partial = pl.pallas_call(
        functools.partial(
            similarity_kernel, len(queries), len(local), cores, groups, members, sources
        ),
        out_shape=jax.ShapeDtypeStruct((devices, rows), jnp.float32),
        in_specs=[vmem] * (len(queries) + len(local) + len(remote)),
        out_specs=vmem,
        name="similarity",
    )(*queries, *local, *remote)
    home = lax.all_to_all(
        partial, ("grp", "mem"), split_axis=0, concat_axis=0, tiled=True
    )
    return jnp.max(home, axis=0)


def solution(mesh):
    in_specs = (P(("grp", "mem"), None), P(("grp", "mem"), None), P(("grp", "mem")))
    out_specs = P(("grp", "mem"))
    return jax.shard_map(body, mesh=mesh, in_specs=in_specs, out_specs=out_specs, check_vma=False)
```

```python
import functools

import jax
import jax.numpy as jnp
from jax import lax
from jax.experimental import pallas as pl
from jax.experimental.pallas import tpu as pltpu
from jax.sharding import PartitionSpec as P


META = 8
QUERIES = 8
SHIFT = 21


def meeting_slots(count):
    slots = []
    for distance in range(1, (count + 1) // 2):
        slots.append([(i, (i + distance) % count) for i in range(count)])
    if count % 2 == 0:
        half = count // 2
        slots.append([(i, i + half) if i % 2 == 0 else (i + half, i) for i in range(half)])
    return slots[::-1]


def prepare_kernel(x_ref, key_ref, out_ref):
    rows = x_ref.shape[0]
    wide = x_ref[...].astype(jnp.float32)
    scale = lax.rsqrt(jnp.sum(wide * wide, axis=1, keepdims=True) + 1e-06)
    out_ref[0:rows, :] = (wide * scale).astype(jnp.bfloat16)
    key = key_ref[...]
    digit = lax.broadcasted_iota(jnp.int32, (META, rows), 0)
    spread = jnp.where(
        digit == 0,
        key & 255,
        jnp.where(digit == 1, (key >> 8) & 255, jnp.where(digit == 2, key >> 16, 0)),
    )
    out_ref[rows : rows + META, :] = jnp.zeros((META, out_ref.shape[1]), jnp.bfloat16)
    out_ref[rows : rows + META, 0:rows] = spread.astype(jnp.float32).astype(jnp.bfloat16)


def keys_of(ref, rows):
    meta = ref[rows : rows + META, 0:rows].astype(jnp.float32)
    key = meta[0:1] + 256.0 * meta[1:2] + 65536.0 * meta[2:3]
    owner = jnp.where(key > 0.0, jnp.floor(meta[2:3] * (1.0 / 32.0)), -1.0)
    return key, owner


def column(row):
    size = row.shape[1]
    return jnp.broadcast_to(row, (size, size)).T


def places_of(members, pairs):
    grp = lax.axis_index("grp")
    mem = lax.axis_index("mem")
    core = mem % 2
    chip = mem // 2
    near = grp ^ (1 + core)
    other_near = grp ^ (2 - core)
    far = grp ^ 3
    row = chip * 2
    queries = [
        grp * members + row + core,
        grp * members + row + 1 - core,
        near * members + row + core,
        near * members + row + 1 - core,
        other_near * members + row + 1 - core,
        other_near * members + row + core,
        far * members + row + core,
        far * members + row + 1 - core,
    ]
    keys = [None]
    for pair in pairs:
        source = jnp.int32(-1)
        for side, table in enumerate(pair):
            for origin, target in table:
                source = jnp.where((core == side) & (chip == target), origin, source)
        for sender in (core, 1 - core):
            keys.append(jnp.where(source < 0, -1, grp * members + source * 2 + sender))
    return queries, keys


def similarity_kernel(groups, n_query, n_key, has_before, members, pairs, *refs):
    queries = dict(zip(n_query, refs))
    keys = dict(zip(n_key, refs[len(n_query) :]))
    out_ref = refs[-1]
    rows = refs[0].shape[0] - META
    query_places, key_places = places_of(members, pairs)
    slot_of = lax.broadcasted_iota(jnp.int32, out_ref.shape, 0)
    result = refs[-2][...] if has_before else jnp.full(out_ref.shape, -1.0, jnp.float32)
    query_keys = {j: keys_of(q, rows) for j, q in queries.items()}
    other_keys = {i: [column(v) for v in keys_of(k, rows)] for i, k in keys.items()}
    best = {}
    back = {}
    for query_list, key_list in groups:
        other_rows = jnp.concatenate([keys[i][0:rows, :] for i in key_list], axis=0)
        for start in range(0, len(query_list), 2):
            some = query_list[start : start + 2]
            query_rows = jnp.concatenate([queries[j][0:rows, :] for j in some], axis=0)
            gram = lax.dot_general(
                other_rows,
                query_rows,
                (((1,), (1,)), ((), ())),
                preferred_element_type=jnp.float32,
            )
            for a, i in enumerate(key_list):
                key, owner = other_keys[i]
                for b, j in enumerate(some):
                    query_key, query_owner = query_keys[j]
                    tile = gram[a * rows : (a + 1) * rows, b * rows : (b + 1) * rows]
                    same = owner == query_owner
                    found = jnp.where(same & (key < query_key), tile, -1.0)
                    best[j] = jnp.maximum(best[j], found) if j in best else found
                    if key_places[i] is not None:
                        found = jnp.where(same & (query_key < key), tile, -1.0)
                        back[i] = jnp.maximum(back[i], found) if i in back else found
    maxima = [(query_places[j], value) for j, value in best.items()]
    maxima += [(key_places[i], value.T) for i, value in back.items()]
    for place, value in maxima:
        result = jnp.maximum(
            result,
            jnp.where(slot_of == place, jnp.max(value, axis=0, keepdims=True), -1.0),
        )
    out_ref[...] = result


def body(embeddings, cluster, rank):
    rows, width = embeddings.shape
    groups = lax.axis_size("grp")
    members = lax.axis_size("mem")
    chips = members // 2
    devices = groups * members
    vmem = pl.BlockSpec(memory_space=pltpu.VMEM)
    key = cluster[:, 0] * (1 << SHIFT) + rank + 1
    block = pl.pallas_call(
        prepare_kernel,
        out_shape=jax.ShapeDtypeStruct((rows + META, width), jnp.bfloat16),
        in_specs=[vmem] * 2,
        out_specs=vmem,
        compiler_params=pltpu.CompilerParams(vmem_limit_bytes=4 << 20),
        name="prepare",
    )(embeddings, key.reshape(1, rows))

    def send(value, route):
        return lax.ppermute(value, ("grp", "mem"), route)

    def swap(value):
        return send(value, [(i, i ^ 1) for i in range(devices)])

    def across(step):
        return [
            (g * members + m, (g ^ step[m % 2]) * members + m)
            for g in range(groups)
            for m in range(members)
        ]

    def along(pair):
        return [
            (g * members + 2 * a + c, g * members + 2 * b + c)
            for g in range(groups)
            for c, slot in enumerate(pair)
            for a, b in slot
        ]

    slots = meeting_slots(chips)
    slots += [[]] * (len(slots) % 2)
    pairs = [slots[i : i + 2] for i in range(0, len(slots), 2)]
    partner = swap(block)
    near = send(block, across((1, 2)))
    near_partner = send(partner, across((1, 2)))
    far = send(near, across((2, 1)))
    keys = [block]
    for pair in pairs:
        keys.append(send(block, along(pair)))
        keys.append(send(partner, along(pair)))
    queries = [
        block,
        partner,
        near,
        near_partner,
        swap(near),
        swap(near_partner),
        far,
        swap(far),
    ]

    def maxima(work, before):
        used_queries = sorted({j for some, _ in work for j in some})
        used_keys = sorted({i for _, some in work for i in some})
        operands = [queries[j] for j in used_queries] + [keys[i] for i in used_keys]
        operands += [] if before is None else [before]
        products = sum(len(some) * len(other) for some, other in work)
        return pl.pallas_call(
            functools.partial(
                similarity_kernel,
                work,
                used_queries,
                used_keys,
                before is not None,
                members,
                pairs,
            ),
            out_shape=jax.ShapeDtypeStruct((devices, rows), jnp.float32),
            in_specs=[vmem] * len(operands),
            out_specs=vmem,
            compiler_params=pltpu.CompilerParams(vmem_limit_bytes=16 << 20),
            cost_estimate=pl.CostEstimate(
                flops=2 * products * rows * rows * width,
                bytes_accessed=0,
                transcendentals=0,
            ),
        )(*operands)

    last = len(keys) - 1
    near_queries = list(range(QUERIES - 2))
    first = list(range(last))
    found = maxima([(near_queries, first)], None)
    found = maxima([([QUERIES - 2, QUERIES - 1], first)], found)
    found = maxima([(list(range(QUERIES)), [last])], found)
    home = lax.all_to_all(
        found, ("grp", "mem"), split_axis=0, concat_axis=0, tiled=True
    )
    return jnp.max(home, axis=0)


def solution(mesh):
    in_specs = (P(("grp", "mem"), None), P(("grp", "mem"), None), P(("grp", "mem")))
    out_specs = P(("grp", "mem"))
    return jax.shard_map(
        body, mesh=mesh, in_specs=in_specs, out_specs=out_specs, check_vma=False
    )
```

```python
import functools

import jax
import jax.numpy as jnp
from jax import lax
from jax.experimental import pallas as pl
from jax.experimental.pallas import tpu as pltpu
from jax.sharding import PartitionSpec as P


META = 16
QUERIES = 8
CHUNKS = 4
SHIFT = 21


def meeting_slots(count):
    slots = []
    for distance in range(1, (count + 1) // 2):
        slots.append([(i, (i + distance) % count) for i in range(count)])
    if count % 2 == 0:
        half = count // 2
        slots.append([(i, i + half) if i % 2 == 0 else (i + half, i) for i in range(half)])
    return slots[::-1]


def prepare_kernel(x_ref, cluster_ref, rank_ref, out_ref, x_buf, meta_buf, sems):
    rows = x_ref.shape[0]
    part = rows // CHUNKS
    loads = [
        pltpu.make_async_copy(
            x_ref.at[pl.ds(i * part, part), :],
            x_buf.at[pl.ds(i * part, part), :],
            sems.at[i],
        )
        for i in range(CHUNKS)
    ]
    loads.append(pltpu.make_async_copy(cluster_ref, meta_buf.at[0], sems.at[CHUNKS]))
    loads.append(pltpu.make_async_copy(rank_ref, meta_buf.at[1], sems.at[CHUNKS + 1]))
    for load in loads:
        load.start()
    width = x_ref.shape[1]
    for i in range(CHUNKS):
        loads[i].wait()
        wide = x_buf[i * part : (i + 1) * part, :].astype(jnp.float32)
        scale = lax.rsqrt(jnp.sum(wide * wide, axis=1, keepdims=True) + 1e-06)
        narrow = (wide * scale).astype(jnp.bfloat16)
        for start in range(0, width, rows):
            out_ref[start + i * part : start + (i + 1) * part, :] = narrow[
                :, start : start + rows
            ]
    loads[CHUNKS].wait()
    loads[CHUNKS + 1].wait()
    key = meta_buf[0] * (1 << SHIFT) + meta_buf[1] + 1
    digit = lax.broadcasted_iota(jnp.int32, (META, rows), 0)
    spread = jnp.where(
        digit == 0,
        key & 255,
        jnp.where(digit == 1, (key >> 8) & 255, jnp.where(digit == 2, key >> 16, 0)),
    )
    out_ref[width : width + META, :] = spread.astype(jnp.float32).astype(jnp.bfloat16)


def rows_of(ref):
    rows = ref.shape[1]
    return jnp.concatenate(
        [ref[i : i + rows, :] for i in range(0, ref.shape[0] - META, rows)], axis=1
    )


def keys_of(ref):
    meta = ref[ref.shape[0] - META :, :].astype(jnp.float32)
    key = meta[0:1] + 256.0 * meta[1:2] + 65536.0 * meta[2:3]
    owner = jnp.where(key > 0.0, jnp.floor(meta[2:3] * (1.0 / 32.0)), -1.0)
    return key, owner


def column(row):
    size = row.shape[1]
    return jnp.broadcast_to(row, (size, size)).T


def places_of(members, pairs):
    grp = lax.axis_index("grp")
    mem = lax.axis_index("mem")
    core = mem % 2
    chip = mem // 2
    near = grp ^ (1 + core)
    other_near = grp ^ (2 - core)
    far = grp ^ 3
    row = chip * 2
    queries = [
        grp * members + row + core,
        grp * members + row + 1 - core,
        near * members + row + core,
        near * members + row + 1 - core,
        other_near * members + row + 1 - core,
        other_near * members + row + core,
        far * members + row + core,
        far * members + row + 1 - core,
    ]
    keys = [None]
    for pair in pairs:
        source = jnp.int32(-1)
        for side, table in enumerate(pair):
            for origin, target in table:
                source = jnp.where((core == side) & (chip == target), origin, source)
        for sender in (core, 1 - core):
            keys.append(jnp.where(source < 0, -1, grp * members + source * 2 + sender))
    return queries, keys


def similarity_kernel(groups, n_query, n_key, has_before, members, pairs, *refs):
    queries = dict(zip(n_query, refs))
    keys = dict(zip(n_key, refs[len(n_query) :]))
    out_ref = refs[-1]
    rows = refs[0].shape[1]
    query_places, key_places = places_of(members, pairs)
    slot_of = lax.broadcasted_iota(jnp.int32, out_ref.shape, 0)
    result = refs[-2][...] if has_before else jnp.full(out_ref.shape, -1.0, jnp.float32)
    query_keys = {j: keys_of(q) for j, q in queries.items()}
    other_keys = {i: [column(v) for v in keys_of(k)] for i, k in keys.items()}
    best = {}
    back = {}
    for query_list, key_list in groups:
        other_rows = jnp.concatenate([rows_of(keys[i]) for i in key_list], axis=0)
        for start in range(0, len(query_list), 2):
            some = query_list[start : start + 2]
            query_rows = jnp.concatenate([rows_of(queries[j]) for j in some], axis=0)
            gram = lax.dot_general(
                other_rows,
                query_rows,
                (((1,), (1,)), ((), ())),
                preferred_element_type=jnp.float32,
            )
            for a, i in enumerate(key_list):
                key, owner = other_keys[i]
                for b, j in enumerate(some):
                    query_key, query_owner = query_keys[j]
                    tile = gram[a * rows : (a + 1) * rows, b * rows : (b + 1) * rows]
                    same = owner == query_owner
                    found = jnp.where(same & (key < query_key), tile, -1.0)
                    best[j] = jnp.maximum(best[j], found) if j in best else found
                    if key_places[i] is not None:
                        found = jnp.where(same & (query_key < key), tile, -1.0)
                        back[i] = jnp.maximum(back[i], found) if i in back else found
    maxima = [(query_places[j], value) for j, value in best.items()]
    maxima += [(key_places[i], value.T) for i, value in back.items()]
    for place, value in maxima:
        result = jnp.maximum(
            result,
            jnp.where(slot_of == place, jnp.max(value, axis=0, keepdims=True), -1.0),
        )
    out_ref[...] = result


def body(embeddings, cluster, rank):
    rows, width = embeddings.shape
    groups = lax.axis_size("grp")
    members = lax.axis_size("mem")
    chips = members // 2
    devices = groups * members
    vmem = pl.BlockSpec(memory_space=pltpu.VMEM)
    anywhere = pl.BlockSpec(memory_space=pl.ANY)
    block = pl.pallas_call(
        prepare_kernel,
        out_shape=jax.ShapeDtypeStruct((width + META, rows), jnp.bfloat16),
        in_specs=[anywhere] * 3,
        out_specs=vmem,
        scratch_shapes=[
            pltpu.VMEM((rows, width), jnp.bfloat16),
            pltpu.VMEM((2, 1, rows), jnp.int32),
            pltpu.SemaphoreType.DMA((CHUNKS + 2,)),
        ],
        compiler_params=pltpu.CompilerParams(vmem_limit_bytes=4 << 20),
        name="prepare",
    )(*(
        pltpu.with_memory_space_constraint(value, pltpu.HBM)
        for value in (embeddings, cluster.reshape(1, rows), rank.reshape(1, rows))
    ))

    def send(value, route):
        return lax.ppermute(value, ("grp", "mem"), route)

    def swap(value):
        return send(value, [(i, i ^ 1) for i in range(devices)])

    def across(step):
        return [
            (g * members + m, (g ^ step[m % 2]) * members + m)
            for g in range(groups)
            for m in range(members)
        ]

    def along(pair):
        return [
            (g * members + 2 * a + c, g * members + 2 * b + c)
            for g in range(groups)
            for c, slot in enumerate(pair)
            for a, b in slot
        ]

    slots = meeting_slots(chips)
    slots += [[]] * (len(slots) % 2)
    pairs = [slots[i : i + 2] for i in range(0, len(slots), 2)]
    partner = swap(block)
    near = send(block, across((1, 2)))
    near_partner = send(partner, across((1, 2)))
    far = send(near, across((2, 1)))
    keys = [block]
    for pair in pairs:
        keys.append(send(block, along(pair)))
        keys.append(send(partner, along(pair)))
    queries = [
        block,
        partner,
        near,
        near_partner,
        swap(near),
        swap(near_partner),
        far,
        swap(far),
    ]

    def maxima(work, before):
        used_queries = sorted({j for some, _ in work for j in some})
        used_keys = sorted({i for _, some in work for i in some})
        operands = [queries[j] for j in used_queries] + [keys[i] for i in used_keys]
        operands += [] if before is None else [before]
        products = sum(len(some) * len(other) for some, other in work)
        return pl.pallas_call(
            functools.partial(
                similarity_kernel,
                work,
                used_queries,
                used_keys,
                before is not None,
                members,
                pairs,
            ),
            out_shape=jax.ShapeDtypeStruct((devices, rows), jnp.float32),
            in_specs=[vmem] * len(operands),
            out_specs=vmem,
            compiler_params=pltpu.CompilerParams(vmem_limit_bytes=16 << 20),
            cost_estimate=pl.CostEstimate(
                flops=2 * products * rows * rows * width,
                bytes_accessed=0,
                transcendentals=0,
            ),
        )(*operands)

    last = len(keys) - 1
    near_queries = list(range(QUERIES - 2))
    first = list(range(last))
    found = maxima([(near_queries, first)], None)
    found = maxima([([QUERIES - 2], first)], found)
    found = maxima([(list(range(QUERIES - 1)), [last])], found)
    found = maxima([([QUERIES - 1], first + [last])], found)
    home = lax.all_to_all(
        found, ("grp", "mem"), split_axis=0, concat_axis=0, tiled=True
    )
    return jnp.max(home, axis=0)


def solution(mesh):
    in_specs = (P(("grp", "mem"), None), P(("grp", "mem"), None), P(("grp", "mem")))
    out_specs = P(("grp", "mem"))
    return jax.shard_map(
        body, mesh=mesh, in_specs=in_specs, out_specs=out_specs, check_vma=False
    )
```

```python
import functools

import jax
import jax.numpy as jnp
from jax import lax
from jax.experimental import pallas as pl
from jax.experimental.pallas import tpu as pltpu
from jax.sharding import PartitionSpec as P


META = 16
QUERIES = 8
SHIFT = 21


def meeting_slots(count):
    slots = []
    for distance in range(1, (count + 1) // 2):
        slots.append([(i, (i + distance) % count) for i in range(count)])
    if count % 2 == 0:
        half = count // 2
        slots.append([(i, i + half) if i % 2 == 0 else (i + half, i) for i in range(half)])
    return slots[::-1]


def prepare_kernel(x_ref, cluster_ref, rank_ref, out_ref, x_buf, meta_buf, sems):
    rows, width = x_ref.shape
    loads = [
        pltpu.make_async_copy(x_ref, x_buf, sems.at[0]),
        pltpu.make_async_copy(cluster_ref, meta_buf.at[0], sems.at[1]),
        pltpu.make_async_copy(rank_ref, meta_buf.at[1], sems.at[2]),
    ]
    for load in loads:
        load.start()
    for load in loads:
        load.wait()
    wide = x_buf[...].astype(jnp.float32)
    scale = lax.rsqrt(jnp.sum(wide * wide, axis=1, keepdims=True) + 1e-06)
    normed = (wide * scale).astype(jnp.bfloat16)
    for start in range(0, width, rows):
        out_ref[start : start + rows, :] = normed[:, start : start + rows]
    key = meta_buf[0] * (1 << SHIFT) + meta_buf[1] + 1
    digit = lax.broadcasted_iota(jnp.int32, (META, rows), 0)
    spread = jnp.where(
        digit == 0,
        key & 255,
        jnp.where(digit == 1, (key >> 8) & 255, jnp.where(digit == 2, key >> 16, 0)),
    )
    out_ref[width : width + META, :] = spread.astype(jnp.float32).astype(jnp.bfloat16)


def rows_of(ref):
    rows = ref.shape[1]
    return jnp.concatenate(
        [ref[i : i + rows, :] for i in range(0, ref.shape[0] - META, rows)], axis=1
    )


def keys_of(ref):
    meta = ref[ref.shape[0] - META :, :].astype(jnp.float32)
    key = meta[0:1] + 256.0 * meta[1:2] + 65536.0 * meta[2:3]
    owner = jnp.where(key > 0.0, jnp.floor(meta[2:3] * (1.0 / 32.0)), -1.0)
    return key, owner


def column(row):
    size = row.shape[1]
    return jnp.broadcast_to(row, (size, size)).T


def places_of(members, pairs):
    grp = lax.axis_index("grp")
    mem = lax.axis_index("mem")
    core = mem % 2
    chip = mem // 2
    near = grp ^ (1 + core)
    other_near = grp ^ (2 - core)
    far = grp ^ 3
    row = chip * 2
    queries = [
        grp * members + row + core,
        grp * members + row + 1 - core,
        near * members + row + core,
        near * members + row + 1 - core,
        other_near * members + row + 1 - core,
        other_near * members + row + core,
        far * members + row + core,
        far * members + row + 1 - core,
    ]
    keys = [None]
    for pair in pairs:
        source = jnp.int32(-1)
        for side, table in enumerate(pair):
            for origin, target in table:
                source = jnp.where((core == side) & (chip == target), origin, source)
        for sender in (core, 1 - core):
            keys.append(jnp.where(source < 0, -1, grp * members + source * 2 + sender))
    return queries, keys


def similarity_kernel(groups, n_query, n_key, has_before, members, pairs, *refs):
    queries = dict(zip(n_query, refs))
    keys = dict(zip(n_key, refs[len(n_query) :]))
    out_ref = refs[-1]
    rows = refs[0].shape[1]
    query_places, key_places = places_of(members, pairs)
    slot_of = lax.broadcasted_iota(jnp.int32, out_ref.shape, 0)
    result = refs[-2][...] if has_before else jnp.full(out_ref.shape, -1.0, jnp.float32)
    upright = len(queries) < len(keys)
    query_keys = {j: keys_of(q) for j, q in queries.items()}
    other_keys = {i: keys_of(k) for i, k in keys.items()}
    tall = query_keys if upright else other_keys
    for name, pair in tall.items():
        tall[name] = [column(value) for value in pair]
    best = {}
    back = {}

    def gather(found, name, mask, tile):
        tile = jnp.where(mask, tile, -1.0)
        found[name] = jnp.maximum(found[name], tile) if name in found else tile

    def panel(blocks, names):
        return jnp.concatenate([rows_of(blocks[name]) for name in names], axis=0)

    for query_list, key_list in groups:
        down, along = (queries, keys) if upright else (keys, queries)
        down_list, along_list = (
            (query_list, key_list) if upright else (key_list, query_list)
        )
        down_rows = panel(down, down_list)
        for start in range(0, len(along_list), 2):
            some = along_list[start : start + 2]
            gram = lax.dot_general(
                down_rows,
                panel(along, some),
                (((1,), (1,)), ((), ())),
                preferred_element_type=jnp.float32,
            )
            for a, d in enumerate(down_list):
                for b, w in enumerate(some):
                    j, i = (d, w) if upright else (w, d)
                    query_key, query_owner = query_keys[j]
                    key, owner = other_keys[i]
                    tile = gram[a * rows : (a + 1) * rows, b * rows : (b + 1) * rows]
                    same = owner == query_owner
                    gather(best, j, same & (key < query_key), tile)
                    if key_places[i] is not None:
                        gather(back, i, same & (query_key < key), tile)
    maxima = [
        (query_places[j], value.T if upright else value) for j, value in best.items()
    ]
    maxima += [
        (key_places[i], value if upright else value.T) for i, value in back.items()
    ]
    for place, value in maxima:
        result = jnp.maximum(
            result,
            jnp.where(slot_of == place, jnp.max(value, axis=0, keepdims=True), -1.0),
        )
    out_ref[...] = result


def body(embeddings, cluster, rank):
    rows, width = embeddings.shape
    groups = lax.axis_size("grp")
    members = lax.axis_size("mem")
    chips = members // 2
    devices = groups * members
    vmem = pl.BlockSpec(memory_space=pltpu.VMEM)
    anywhere = pl.BlockSpec(memory_space=pl.ANY)
    block = pl.pallas_call(
        prepare_kernel,
        out_shape=jax.ShapeDtypeStruct((width + META, rows), jnp.bfloat16),
        in_specs=[anywhere] * 3,
        out_specs=vmem,
        scratch_shapes=[
            pltpu.VMEM((rows, width), jnp.bfloat16),
            pltpu.VMEM((2, 1, rows), jnp.int32),
            pltpu.SemaphoreType.DMA((3,)),
        ],
        compiler_params=pltpu.CompilerParams(vmem_limit_bytes=4 << 20),
        name="prepare",
    )(*(
        pltpu.with_memory_space_constraint(value, pltpu.HBM)
        for value in (embeddings, cluster.reshape(1, rows), rank.reshape(1, rows))
    ))

    def send(value, route):
        return lax.ppermute(value, ("grp", "mem"), route)

    def swap(value):
        return send(value, [(i, i ^ 1) for i in range(devices)])

    def across(step):
        return [
            (g * members + m, (g ^ step[m % 2]) * members + m)
            for g in range(groups)
            for m in range(members)
        ]

    def along(pair):
        return [
            (g * members + 2 * a + c, g * members + 2 * b + c)
            for g in range(groups)
            for c, slot in enumerate(pair)
            for a, b in slot
        ]

    slots = meeting_slots(chips)
    slots += [[]] * (len(slots) % 2)
    pairs = [slots[i : i + 2] for i in range(0, len(slots), 2)]
    partner = swap(block)
    near = send(block, across((1, 2)))
    near_partner = send(partner, across((1, 2)))
    far = send(near, across((2, 1)))
    keys = [block]
    for pair in pairs:
        keys.append(send(block, along(pair)))
        keys.append(send(partner, along(pair)))
    queries = [
        block,
        partner,
        near,
        near_partner,
        swap(near),
        swap(near_partner),
        far,
        swap(far),
    ]

    def maxima(work, before):
        used_queries = sorted({j for some, _ in work for j in some})
        used_keys = sorted({i for _, some in work for i in some})
        operands = [queries[j] for j in used_queries] + [keys[i] for i in used_keys]
        operands += [] if before is None else [before]
        products = sum(len(some) * len(other) for some, other in work)
        return pl.pallas_call(
            functools.partial(
                similarity_kernel,
                work,
                used_queries,
                used_keys,
                before is not None,
                members,
                pairs,
            ),
            out_shape=jax.ShapeDtypeStruct((devices, rows), jnp.float32),
            in_specs=[vmem] * len(operands),
            out_specs=vmem,
            compiler_params=pltpu.CompilerParams(vmem_limit_bytes=16 << 20),
            cost_estimate=pl.CostEstimate(
                flops=2 * products * rows * rows * width,
                bytes_accessed=0,
                transcendentals=0,
            ),
        )(*operands)

    last = len(keys) - 1
    near_queries = list(range(QUERIES - 2))
    first = list(range(last))
    found = maxima([(near_queries, first)], None)
    found = maxima([([QUERIES - 2], first)], found)
    found = maxima([(list(range(QUERIES - 1)), [last])], found)
    found = maxima([([QUERIES - 1], first + [last])], found)
    home = lax.all_to_all(
        found, ("grp", "mem"), split_axis=0, concat_axis=0, tiled=True
    )
    return jnp.max(home, axis=0)


def solution(mesh):
    in_specs = (P(("grp", "mem"), None), P(("grp", "mem"), None), P(("grp", "mem")))
    out_specs = P(("grp", "mem"))
    return jax.shard_map(
        body, mesh=mesh, in_specs=in_specs, out_specs=out_specs, check_vma=False
    )
```

```python
import functools

import jax
import jax.numpy as jnp
from jax import lax
from jax.experimental import pallas as pl
from jax.experimental.pallas import tpu as pltpu
from jax.sharding import PartitionSpec as P


META = 16
QUERIES = 8
SHIFT = 21


def meeting_slots(count):
    slots = []
    for distance in range(1, (count + 1) // 2):
        slots.append([(i, (i + distance) % count) for i in range(count)])
    if count % 2 == 0:
        half = count // 2
        slots.append([(i, i + half) if i % 2 == 0 else (i + half, i) for i in range(half)])
    return slots[::-1]


def prepare_kernel(x_ref, cluster_ref, rank_ref, out_ref, x_buf, meta_buf, sems):
    rows, width = x_ref.shape
    loads = [
        pltpu.make_async_copy(x_ref, x_buf, sems.at[0]),
        pltpu.make_async_copy(cluster_ref, meta_buf.at[0], sems.at[1]),
        pltpu.make_async_copy(rank_ref, meta_buf.at[1], sems.at[2]),
    ]
    for load in loads:
        load.start()
    for load in loads:
        load.wait()
    wide = x_buf[...].astype(jnp.float32)
    scale = lax.rsqrt(jnp.sum(wide * wide, axis=1, keepdims=True) + 1e-06)
    normed = (wide * scale).astype(jnp.bfloat16)
    for start in range(0, width, rows):
        out_ref[start : start + rows, :] = normed[:, start : start + rows]
    key = meta_buf[0] * (1 << SHIFT) + meta_buf[1] + 1
    digit = lax.broadcasted_iota(jnp.int32, (META, rows), 0)
    spread = jnp.where(
        digit == 0,
        key & 255,
        jnp.where(digit == 1, (key >> 8) & 255, jnp.where(digit == 2, key >> 16, 0)),
    )
    out_ref[width : width + META, :] = spread.astype(jnp.float32).astype(jnp.bfloat16)


def rows_of(ref):
    rows = ref.shape[1]
    return jnp.concatenate(
        [ref[i : i + rows, :] for i in range(0, ref.shape[0] - META, rows)], axis=1
    )


def keys_of(ref):
    meta = ref[ref.shape[0] - META :, :].astype(jnp.float32)
    key = meta[0:1] + 256.0 * meta[1:2] + 65536.0 * meta[2:3]
    owner = jnp.where(key > 0.0, jnp.floor(meta[2:3] * (1.0 / 32.0)), -1.0)
    return key, owner


def column(row):
    size = row.shape[1]
    return jnp.broadcast_to(row, (size, size)).T


def places_of(members, pairs):
    grp = lax.axis_index("grp")
    mem = lax.axis_index("mem")
    core = mem % 2
    chip = mem // 2
    near = grp ^ (2 - core)
    other_near = grp ^ (1 + core)
    far = grp ^ 3
    row = chip * 2
    queries = [
        grp * members + row + core,
        grp * members + row + 1 - core,
        near * members + row + core,
        near * members + row + 1 - core,
        other_near * members + row + 1 - core,
        other_near * members + row + core,
        far * members + row + core,
        far * members + row + 1 - core,
    ]
    keys = [None, None]
    for pair in pairs:
        sources = []
        for mine in (core, 1 - core):
            source = jnp.int32(-1)
            for side, table in enumerate(pair):
                for origin, target in table:
                    source = jnp.where(
                        (mine == side) & (chip == target), origin, source
                    )
            sources.append(source)
        for source, sender in (
            (sources[0], core),
            (sources[1], 1 - core),
            (sources[0], 1 - core),
        ):
            keys.append(jnp.where(source < 0, -1, grp * members + source * 2 + sender))
    return queries, keys


def similarity_kernel(groups, n_query, n_key, has_before, members, pairs, *refs):
    queries = dict(zip(n_query, refs))
    keys = dict(zip(n_key, refs[len(n_query) :]))
    out_ref = refs[-1]
    rows = refs[0].shape[1]
    query_places, key_places = places_of(members, pairs)
    slot_of = lax.broadcasted_iota(jnp.int32, out_ref.shape, 0)
    result = refs[-2][...] if has_before else jnp.full(out_ref.shape, -1.0, jnp.float32)
    upright = len(queries) < len(keys)
    query_keys = {j: keys_of(q) for j, q in queries.items()}
    other_keys = {i: keys_of(k) for i, k in keys.items()}
    tall = query_keys if upright else other_keys
    for name, pair in tall.items():
        tall[name] = [column(value) for value in pair]
    best = {}
    back = {}

    def gather(found, name, mask, tile):
        tile = jnp.where(mask, tile, -1.0)
        found[name] = jnp.maximum(found[name], tile) if name in found else tile

    def panel(blocks, names):
        return jnp.concatenate([rows_of(blocks[name]) for name in names], axis=0)

    for query_list, key_list in groups:
        down, along = (queries, keys) if upright else (keys, queries)
        down_list, along_list = (
            (query_list, key_list) if upright else (key_list, query_list)
        )
        down_rows = panel(down, down_list)
        for start in range(0, len(along_list), 2):
            some = along_list[start : start + 2]
            gram = lax.dot_general(
                down_rows,
                panel(along, some),
                (((1,), (1,)), ((), ())),
                preferred_element_type=jnp.float32,
            )
            for a, d in enumerate(down_list):
                for b, w in enumerate(some):
                    j, i = (d, w) if upright else (w, d)
                    query_key, query_owner = query_keys[j]
                    key, owner = other_keys[i]
                    tile = gram[a * rows : (a + 1) * rows, b * rows : (b + 1) * rows]
                    same = owner == query_owner
                    gather(best, j, same & (key < query_key), tile)
                    if key_places[i] is not None:
                        gather(back, i, same & (query_key < key), tile)
    maxima = [
        (query_places[j], value.T if upright else value) for j, value in best.items()
    ]
    maxima += [
        (key_places[i], value if upright else value.T) for i, value in back.items()
    ]
    for place, value in maxima:
        result = jnp.maximum(
            result,
            jnp.where(slot_of == place, jnp.max(value, axis=0, keepdims=True), -1.0),
        )
    out_ref[...] = result


def body(embeddings, cluster, rank):
    rows, width = embeddings.shape
    groups = lax.axis_size("grp")
    members = lax.axis_size("mem")
    chips = members // 2
    devices = groups * members
    vmem = pl.BlockSpec(memory_space=pltpu.VMEM)
    anywhere = pl.BlockSpec(memory_space=pl.ANY)
    block = pl.pallas_call(
        prepare_kernel,
        out_shape=jax.ShapeDtypeStruct((width + META, rows), jnp.bfloat16),
        in_specs=[anywhere] * 3,
        out_specs=vmem,
        scratch_shapes=[
            pltpu.VMEM((rows, width), jnp.bfloat16),
            pltpu.VMEM((2, 1, rows), jnp.int32),
            pltpu.SemaphoreType.DMA((3,)),
        ],
        compiler_params=pltpu.CompilerParams(vmem_limit_bytes=4 << 20),
        name="prepare",
    )(*(
        pltpu.with_memory_space_constraint(value, pltpu.HBM)
        for value in (embeddings, cluster.reshape(1, rows), rank.reshape(1, rows))
    ))

    def send(value, route):
        return lax.ppermute(value, ("grp", "mem"), route)

    def swap(value):
        return send(value, [(i, i ^ 1) for i in range(devices)])

    def across(step):
        return [
            (g * members + m, (g ^ step[m % 2]) * members + m)
            for g in range(groups)
            for m in range(members)
        ]

    def along(pair):
        return [
            (g * members + 2 * a + c, g * members + 2 * b + c)
            for g in range(groups)
            for c, slot in enumerate(pair)
            for a, b in slot
        ]

    slots = meeting_slots(chips)
    slots += [[]] * (len(slots) % 2)
    pairs = [slots[i : i + 2] for i in range(0, len(slots), 2)]
    partner = swap(block)
    near = send(block, across((2, 1)))
    near_partner = send(partner, across((2, 1)))
    far = send(near, across((1, 2)))
    keys = [block, partner]
    lines = []
    for pair in pairs:
        line = send(block, along(pair))
        keys += [line, swap(line)]
        keys.append(send(partner, along(pair)))
        lines += [len(keys) - 3, len(keys) - 1]
    queries = [
        block,
        partner,
        near,
        near_partner,
        swap(near),
        swap(near_partner),
        far,
        swap(far),
    ]

    def maxima(work, before):
        used_queries = sorted({j for some, _ in work for j in some})
        used_keys = sorted({i for _, some in work for i in some})
        operands = [queries[j] for j in used_queries] + [keys[i] for i in used_keys]
        operands += [] if before is None else [before]
        products = sum(len(some) * len(other) for some, other in work)
        return pl.pallas_call(
            functools.partial(
                similarity_kernel,
                work,
                used_queries,
                used_keys,
                before is not None,
                members,
                pairs,
            ),
            out_shape=jax.ShapeDtypeStruct((devices, rows), jnp.float32),
            in_specs=[vmem] * len(operands),
            out_specs=vmem,
            compiler_params=pltpu.CompilerParams(vmem_limit_bytes=16 << 20),
            cost_estimate=pl.CostEstimate(
                flops=2 * products * rows * rows * width,
                bytes_accessed=0,
                transcendentals=0,
            ),
        )(*operands)

    near_queries = list(range(QUERIES - 2))
    far_query, swapped_query = QUERIES - 2, QUERIES - 1
    shared = [0, 1, lines[0], lines[0] + 1]
    found = maxima([(near_queries, [0] + lines[:-1])], None)
    found = maxima([([far_query], shared + lines[1:-1])], found)
    found = maxima([(near_queries + [far_query], lines[-1:])], found)
    found = maxima([([swapped_query], lines[1:])], found)
    home = lax.all_to_all(
        found, ("grp", "mem"), split_axis=0, concat_axis=0, tiled=True
    )
    return jnp.max(home, axis=0)


def solution(mesh):
    in_specs = (P(("grp", "mem"), None), P(("grp", "mem"), None), P(("grp", "mem")))
    out_specs = P(("grp", "mem"))
    return jax.shard_map(
        body, mesh=mesh, in_specs=in_specs, out_specs=out_specs, check_vma=False
    )
```
